32 devices in a mesh: sy: 4 (over y, x), sx: 4 (over z), wl: 2 (over core).
Axes of the slice: x: 2, y: 2, z: 4, core: 2. Of those that a mesh axis runs over, the one named last changes fastest.
Arguments:
- interface_map: bfloat16 [8, 4, 1536, 2, 1536], P(('wl', 'sy'), 'sx'), parts along dimension 0, may hold values from -0.0625 to 0.0625
- source_trace: float32 [8, 4, 2, 64, 4, 384], P(('wl', 'sy'), 'sx'), parts along dimension 0, may hold values from -6 to 6
- restriction: float32 [8, 4, 2, 32, 4, 384], P(('wl', 'sy'), 'sx'), parts along dimension 0, may hold values from -0.02734375 to 0.02734375
- prolongation: float32 [8, 4, 2, 32, 4, 384], P(('wl', 'sy'), 'sx'), parts along dimension 0, may hold values from -0.109375 to 0.109375
- coarse_inverse: float32 [4, 32, 32], P('wl'), parts along dimension 0, may hold values from -0.75 to 0.75
Outputs:
- traces: float32 [8, 4, 2, 64, 4, 384], P(('wl', 'sy'), 'sx'), parts along dimension 0
- coarse_coef: float32 [4, 64, 32], P('wl'), parts along dimension 0
The draws below stay inside these ranges and needn't reach their ends.
There are 2 independent parts, one for each index of `wl`. The reference program is written for one: setup_inputs(seed, part) draws one part's arguments, and reference() takes and returns one part's arrays. A program takes and returns all parts, laid end to end along the dimension named above; each array names one. Nothing has to cross between parts.
All inputs are finite; a program needn't handle non-finite values.
Results may differ from the reference program's by a relative error of at most 0.0025.
Values sent between devices are 32-bit elements; how exact they have to be, the bound alone decides.
A program may use at most 128 MiB of HBM per device.

```python
import jax
import jax.numpy as jnp
from jax import lax

M = 384
NC = 32
S = 64
ITERS = 6
SUBY = 4
SUBX = 4


def steps_of(stream_key, extent, cuts, low, top_value):
    loudness, own = 1.0, jax.random.fold_in(stream_key, 6)
    for position, parts in cuts:
        draws = jnp.exp(jax.random.uniform(jax.random.fold_in(own, position), (parts,), jnp.float32, low / len(cuts), top_value / len(cuts)))
        loudness = loudness * jnp.repeat(draws, extent[position] // parts).reshape([-1 if axis == position else 1 for axis in range(len(extent))])
    return loudness


def centred(key, extent, width, most, cuts=(), dtype=jnp.bfloat16):
    drawn = jax.random.normal(key, extent, jnp.float32) * width
    if len(cuts) > 0:
        drawn = steps_of(key, extent, cuts, -0.22, 0.18) * drawn
    return jnp.clip(drawn, min=-most, max=most).astype(dtype)


def setup_inputs(seed: int = 0, part: int = 0) -> dict:
    key_list = jax.random.split(jax.random.key(seed), 6)
    own_keys = jax.random.split(jax.random.fold_in(key_list[5], part), 6)
    return {
        "interface_map": centred(own_keys[0], (SUBY, SUBX, 4 * M, 2, 4 * M), (24 * M) ** -0.5, 0.0625, ((0, 4), (1, 4))),
        "source_trace": centred(own_keys[1], (SUBY, SUBX, 2, S, 4, M), 1.0, 6.0, ((0, 4), (1, 4)), jnp.float32),
        "restriction": centred(own_keys[2], (SUBY, SUBX, 2, NC, 4, M), (8 * M * SUBY * SUBX) ** -0.5, 0.02734375, ((0, 4), (1, 4)), jnp.float32),
        "prolongation": centred(own_keys[3], (SUBY, SUBX, 2, NC, 4, M), (96 * NC) ** -0.5, 0.109375, ((0, 4), (1, 4)), jnp.float32),
        "coarse_inverse": centred(own_keys[4], (2, NC, NC), (2 * NC) ** -0.5, 0.75, (), jnp.float32),
    }


PRECISE = lax.Precision.HIGHEST


def shifted(values, along, offset):
    length_axis = values.shape[along]
    blank_edge = jnp.zeros_like(lax.slice_in_dim(values, 0, 1, axis=along))
    if offset == 1:
        return jnp.concatenate([blank_edge, lax.slice_in_dim(values, 0, length_axis - 1, axis=along)], axis=along)
    return jnp.concatenate([lax.slice_in_dim(values, 1, length_axis, axis=along), blank_edge], axis=along)


def complex_pair(left_real, left_imag, right_real, right_imag, pattern):
    real_part = jnp.einsum(pattern, left_real, right_real, precision=PRECISE) - jnp.einsum(pattern, left_imag, right_imag, precision=PRECISE)
    imag_part = jnp.einsum(pattern, left_real, right_imag, precision=PRECISE) + jnp.einsum(pattern, left_imag, right_real, precision=PRECISE)
    return jnp.stack([real_part, imag_part])


def corner_values(outgoing):
    corner_northwest = outgoing[..., 0, 0] + outgoing[..., 2, 0]
    corner_northeast = outgoing[..., 0, -1] + outgoing[..., 3, 0]
    corner_southwest = outgoing[..., 1, 0] + outgoing[..., 2, -1]
    corner_southeast = outgoing[..., 1, -1] + outgoing[..., 3, -1]
    return corner_northwest, corner_northeast, corner_southwest, corner_southeast


def assemble(from_north, from_south, from_west, from_east, into_northwest, into_northeast, into_southwest, into_southeast):
    north_side = from_north.at[..., 0].add(0.5 * into_northwest).at[..., -1].add(0.5 * into_northeast)
    south_side = from_south.at[..., 0].add(0.5 * into_southwest).at[..., -1].add(0.5 * into_southeast)
    west_side = from_west.at[..., 0].add(0.5 * into_northwest).at[..., -1].add(0.5 * into_southwest)
    east_side = from_east.at[..., 0].add(0.5 * into_northeast).at[..., -1].add(0.5 * into_southeast)
    return jnp.stack([north_side, south_side, west_side, east_side], axis=-2)


def reference(interface_map, source_trace, restriction, prolongation, coarse_inverse):
    grid_rows, grid_cols = source_trace.shape[0], source_trace.shape[1]
    src_count, side_len = source_trace.shape[3], source_trace.shape[5]
    coarse_width = restriction.shape[3]
    flat_map = interface_map.reshape(grid_rows * grid_cols, 4 * side_len, 8 * side_len)
    rest_flat = restriction.reshape(grid_rows, grid_cols, 2, coarse_width, 4 * side_len)
    lift_flat = prolongation.reshape(grid_rows, grid_cols, 2, coarse_width, 4 * side_len)
    traces = jnp.zeros(source_trace.shape, jnp.float32)
    coef_now = jnp.zeros((2, src_count, coarse_width), jnp.float32)
    for sweep_index in range(ITERS):
        flat_traces = traces.reshape(grid_rows, grid_cols, 2, src_count, 4 * side_len)
        coarse_total = complex_pair(flat_traces[:, :, 0], flat_traces[:, :, 1], rest_flat[:, :, 0], rest_flat[:, :, 1], "yxsk,yxnk->sn")
        coef_now = complex_pair(coarse_total[0], coarse_total[1], coarse_inverse[0], coarse_inverse[1], "sn,nq->sq")
        spread = complex_pair(coef_now[0], coef_now[1], lift_flat[:, :, 0], lift_flat[:, :, 1], "sn,yxnk->yxsk")
        corrected = flat_traces + jnp.moveaxis(spread, 0, 2)
        row_block = corrected.astype(jnp.bfloat16).reshape(grid_rows * grid_cols, 2 * src_count, 4 * side_len)
        product = lax.map(lambda operands: jnp.dot(operands[0], operands[1], preferred_element_type=jnp.float32), (row_block, flat_map))
        product = product.reshape(grid_rows, grid_cols, 2, src_count, 2, 4 * side_len)
        real_part = product[:, :, 0, :, 0] - product[:, :, 1, :, 1]
        imag_part = product[:, :, 0, :, 1] + product[:, :, 1, :, 0]
        outgoing = jnp.stack([real_part, imag_part], axis=2).reshape(source_trace.shape) + source_trace
        from_north = shifted(outgoing[:, :, :, :, 1], 0, 1)
        from_south = shifted(outgoing[:, :, :, :, 0], 0, -1)
        from_west = shifted(outgoing[:, :, :, :, 3], 1, 1)
        from_east = shifted(outgoing[:, :, :, :, 2], 1, -1)
        corner_northwest, corner_northeast, corner_southwest, corner_southeast = corner_values(outgoing)
        into_northwest = shifted(shifted(corner_southeast, 0, 1), 1, 1)
        into_northeast = shifted(shifted(corner_southwest, 0, 1), 1, -1)
        into_southwest = shifted(shifted(corner_northeast, 0, -1), 1, 1)
        into_southeast = shifted(shifted(corner_northwest, 0, -1), 1, -1)
        traces = assemble(from_north, from_south, from_west, from_east, into_northwest, into_northeast, into_southwest, into_southeast)
    return traces, coef_now
```

```python
import functools

import jax
import jax.numpy as jnp
from jax import lax
from jax.experimental import pallas as pl
from jax.experimental.pallas import tpu as pltpu
from jax.sharding import PartitionSpec as P

ITERS = 6
LANES = 128
F32, BF16 = jnp.float32, jnp.bfloat16
MESH = pl.DeviceIdType.MESH
PRECISE = lax.Precision.HIGHEST
NT = (((1,), (1,)), ((), ()))
PARTS = 4


def dot(a, b):
    return jnp.dot(a, b, preferred_element_type=F32)


def dot_nt(a, b):
    return lax.dot_general(a, b, NT, preferred_element_type=F32)


def split(x):
    hi = x.astype(BF16)
    return hi, (x - hi.astype(F32)).astype(BF16)


def sweep_kernel(
    ny, nx, iters,
    map_hbm, src_ref, rest_ref, lift_ref, inv_ref,
    traces_ref, coef_ref,
    stage, table, abuf, apbuf, recv, cbuf, crecv, lhs, ext_lhs, ext_rhs, eap_rhs,
    wts, part, xs, rowsum, ys, inv_full, prev,
    side_send, side_recv, diag_send, diag_recv,
    x_send, x_recv, y_send, y_recv, map_sem,
):
    _, nsrc, k = src_ref.shape
    side = k // 4
    rows = rest_ref.shape[0]
    nc = rows // 2
    gs = nc
    groups = nsrc // gs
    tiles = k // LANES
    half = gs // 2
    ap_slot = 2 * groups
    y, x = lax.axis_index("sy"), lax.axis_index("sx")
    up, dn, lf, rt = y > 0, y < ny - 1, x > 0, x < nx - 1
    odd = lax.rem(y, 2) == 1
    sides = ((up, -1, 0), (dn, 1, 0), (lf, 0, -1), (rt, 0, 1))
    diags = (
        (up & lf, -1, -1),
        (up & rt, -1, 1),
        (dn & lf, 1, -1),
        (dn & rt, 1, 1),
    )

    def lanes(s):
        return pl.ds(s * side, side)

    kpart = k // PARTS

    def map_copy(h, c):
        at = pl.ds(h * kpart, kpart)
        return pltpu.make_async_copy(map_hbm.at[at, c], stage.at[c, at], map_sem.at[h, c])

    for h in range(PARTS):
        for c in range(tiles):
            map_copy(h, c).start()

    def exchange(slot, src):
        flat, diag, flat_in, diag_in = [], [], [], []
        for d, (cond, dy, dx) in enumerate(sides):
            o = d ^ 1
            dev = {"sy": y + dy, "sx": x + dx}
            flat.append((cond, pltpu.make_async_remote_copy(
                src.at[:, :, lanes(d)], recv.at[slot, :, :, lanes(o)],
                side_send.at[slot, d], side_recv.at[slot, o],
                device_id=dev, device_id_type=MESH)))
            flat_in.append((cond, pltpu.make_async_remote_copy(
                src.at[:, :, lanes(d)], recv.at[slot, :, :, lanes(d)],
                side_send.at[slot, d], side_recv.at[slot, d],
                device_id=dev, device_id_type=MESH)))
        for d, (cond, dy, dx) in enumerate(diags):
            o = 3 - d
            dev = {"sy": y + dy, "sx": x + dx}
            diag.append((cond, pltpu.make_async_remote_copy(
                cbuf.at[slot], crecv.at[slot, o], diag_send.at[slot, d], diag_recv.at[slot, o],
                device_id=dev, device_id_type=MESH)))
            diag_in.append((cond, pltpu.make_async_remote_copy(
                cbuf.at[slot], crecv.at[slot, d], diag_send.at[slot, d], diag_recv.at[slot, d],
                device_id=dev, device_id_type=MESH)))
        return flat, diag, flat_in, diag_in

    def each(items, what):
        for cond, c in items:
            pl.when(cond)(getattr(c, what))

    def send(slot, src):
        flat, diag, _, _ = exchange(slot, src)
        each(diag, "start")
        (_, north), (_, south), west, east = flat
        pl.when(dn & odd)(south.start)
        pl.when(up)(north.start)
        pl.when(dn & jnp.logical_not(odd))(south.start)
        each((west, east), "start")

    def wait_in(slot, src):
        _, _, flat_in, diag_in = exchange(slot, src)
        each(diag_in, "wait_recv")
        each(flat_in, "wait_recv")

    def wait_sent(slot, src):
        flat, diag, _, _ = exchange(slot, src)
        each(flat, "wait_send")
        each(diag, "wait_send")

    def pack_corners(read, dst):
        def column(s, last):
            if last:
                return read((s + 1) * side - LANES)[:, LANES - 1:]
            return read(s * side)[:, 0:1]

        lane = lax.broadcasted_iota(jnp.int32, (rows, LANES), 1)
        block = jnp.zeros((rows, LANES), F32)
        for j, (a, b) in enumerate((
            ((0, 0), (2, 0)), ((0, 1), (3, 0)), ((1, 0), (2, 1)), ((1, 1), (3, 1)),
        )):
            block = jnp.where(lane == j, column(*a) + column(*b), block)
        if rows < LANES:
            block = jnp.concatenate([block, jnp.zeros((LANES - rows, LANES), F32)], axis=0)
        dst[...] = block.T[:8]

    def assemble(slot, write):
        row = lax.broadcasted_iota(jnp.int32, (LANES, LANES), 0)
        block = jnp.zeros((LANES, LANES), F32)
        for j in range(4):
            block = jnp.where(row == j, crecv[slot, j][3 - j:4 - j], block)
        cols = block.T[:rows] * 0.5
        lane = lax.broadcasted_iota(jnp.int32, (rows, LANES), 1)
        ends = ((0, 1), (2, 3), (0, 2), (1, 3))
        for s in range(4):
            for t in range(side // LANES):
                at = s * side + t * LANES
                v = recv[slot, :, :, at:at + LANES].reshape(rows, LANES)
                if t == 0:
                    j = ends[s][0]
                    v = v + jnp.where(lane == 0, cols[:, j:j + 1], 0.0)
                if t == side // LANES - 1:
                    j = ends[s][1]
                    v = v + jnp.where(lane == LANES - 1, cols[:, j:j + 1], 0.0)
                write(at, v)

    def store_lhs(at, v):
        hi, lo = split(v)
        lhs[:rows, at:at + LANES] = hi
        lhs[rows:, at:at + LANES] = lo

    def x_copies(i):
        res = []
        for d in range(1, nx):
            dev = {"sy": y, "sx": lax.rem(x + d, nx)}
            res.append((
                pltpu.make_async_remote_copy(
                    part.at[i], xs.at[i, x], x_send.at[i, d], x_recv.at[i, d],
                    device_id=dev, device_id_type=MESH),
                pltpu.make_async_remote_copy(
                    part.at[i], xs.at[i, lax.rem(x + nx - d, nx)], x_send.at[i, d], x_recv.at[i, d],
                    device_id=dev, device_id_type=MESH)))
        return res

    def y_copies(i):
        res = []
        for d in range(1, ny):
            dev = {"sy": lax.rem(y + d, ny), "sx": x}
            res.append((
                pltpu.make_async_remote_copy(
                    rowsum.at[i], ys.at[i, y], y_send.at[i, d], y_recv.at[i, d],
                    device_id=dev, device_id_type=MESH),
                pltpu.make_async_remote_copy(
                    rowsum.at[i], ys.at[i, lax.rem(y + ny - d, ny)], y_send.at[i, d], y_recv.at[i, d],
                    device_id=dev, device_id_type=MESH)))
        return res

    def restrict_start(i):
        t = dot_nt(lhs[...], wts[...])
        t = t[:rows] + t[rows:]
        t = t + pltpu.roll(t, 2 * nc, 1)
        im = pltpu.roll(t[gs:], nc, 1)
        lane = lax.broadcasted_iota(jnp.int32, (gs, LANES), 1)
        t = t[:gs] + jnp.where((lane < nc) | ((lane >= 2 * nc) & (lane < 3 * nc)), -im, im)
        lane = lax.broadcasted_iota(jnp.int32, (half, LANES), 1)
        t = jnp.where(lane < 2 * nc, t[:half], t[half:])
        part[i] = t
        xs[i, x] = t
        for c, _ in x_copies(i):
            c.start()

    def restrict_turn(i):
        for _, c in x_copies(i):
            c.wait_recv()
        t = xs[i, 0]
        for j in range(1, nx):
            t = t + xs[i, j]
        rowsum[i] = t
        ys[i, y] = t
        for c, _ in y_copies(i):
            c.start()

    def restrict_end(i):
        for _, c in y_copies(i):
            c.wait_recv()
        for c, _ in x_copies(i):
            c.wait_send()
        for c, _ in y_copies(i):
            c.wait_send()
        t = ys[i, 0]
        for j in range(1, ny):
            t = t + ys[i, j]
        lane = lax.broadcasted_iota(jnp.int32, (half, LANES), 1)
        low = lane < 2 * nc
        return jnp.concatenate([jnp.where(low, t, 0.0), jnp.where(low, 0.0, t)], axis=0)

    def coarse(i, g):
        t = jnp.concatenate([restrict_end(i), prev[g]], axis=1)
        c_re = jnp.dot(t, inv_full[0], preferred_element_type=F32, precision=PRECISE)
        c_im = jnp.dot(t, inv_full[1], preferred_element_type=F32, precision=PRECISE)
        lane = lax.broadcasted_iota(jnp.int32, (gs, LANES), 1)
        prev[g] = jnp.where(lane < nc, c_re, jnp.where(lane < 2 * nc, c_im, 0.0))
        c = jnp.concatenate([c_re, c_im], axis=0)
        hi, lo = split(c)
        lane = lax.broadcasted_iota(jnp.int32, (rows, LANES), 1)
        mid = (lane >= nc) & (lane < 2 * nc)
        ext_lhs[g] = jnp.where(mid, lo.astype(F32), hi.astype(F32)).astype(BF16)
        return c_re, c_im

    def feedback(i):
        t = restrict_end(i)
        g_re = jnp.dot(t, inv_full[0, :LANES], preferred_element_type=F32, precision=PRECISE)
        g_im = jnp.dot(t, inv_full[1, :LANES], preferred_element_type=F32, precision=PRECISE)
        inv_full[0, LANES:LANES + nc] = g_re
        inv_full[0, LANES + nc:LANES + 2 * nc] = -g_im
        inv_full[1, LANES:LANES + nc] = g_im
        inv_full[1, LANES + nc:LANES + 2 * nc] = g_re

    def combine(w):
        p, q = w[:, :side], w[:, side:]
        return p[:nc] - q[nc:], q[:nc] + p[nc:]

    def cols(s):
        return pl.ds(s * 2 * side, 2 * side)

    def wide_product(write):
        for s in range(4):
            w = dot(lhs[...], table[:, cols(s)])
            re, im = combine(w[:rows] + w[rows:])
            write(s, re, im)

    def stack_rhs(dst, s, re, im):
        for at, v in ((0, re), (side, im)):
            hi, lo = split(v)
            dst[:, s * 2 * side + at:s * 2 * side + at + side] = jnp.concatenate(
                [hi, hi, lo, jnp.zeros((LANES - 3 * nc, side), BF16)], axis=0)

    for d, (cond, _, _) in enumerate(sides):
        @pl.when(jnp.logical_not(cond))
        def _(d=d):
            for slot in range(2 * groups + 1):
                recv[slot, :, :, lanes(d)] = jnp.zeros((2, gs, side), F32)
    for d, (cond, _, _) in enumerate(diags):
        @pl.when(jnp.logical_not(cond))
        def _(d=d):
            for slot in range(2 * groups + 1):
                crecv[slot, d] = jnp.zeros((8, LANES), F32)

    def source(g):
        return src_ref.at[:, pl.ds(g * gs, gs)]

    for g in range(groups):
        pack_corners(
            lambda at, g=g: src_ref[:, g * gs:(g + 1) * gs, at:at + LANES].reshape(rows, LANES),
            cbuf.at[g])
        send(g, source(g))

    cr, ci = inv_ref[0], inv_ref[1]
    blank = jnp.zeros((nc, LANES - 3 * nc), F32)
    for i, (top, bottom) in enumerate(((cr, -ci), (ci, cr))):
        for j, v in enumerate((top, bottom, top, bottom)):
            inv_full[i, j * nc:(j + 1) * nc] = jnp.concatenate([v, v, v, blank], axis=1)
        inv_full[i, LANES:] = jnp.zeros((LANES, LANES), F32)
    prev[...] = jnp.zeros_like(prev)
    hi, lo = split(rest_ref[...])
    wts[:rows] = hi
    wts[rows:] = lo
    hi, lo = split(lift_ref[...])
    lhs[:rows] = hi
    lhs[rows:] = lo

    r = lax.broadcasted_iota(jnp.int32, (2 * LANES, 2 * LANES), 0)
    c = lax.broadcasted_iota(jnp.int32, (2 * LANES, 2 * LANES), 1)
    pick = jnp.where(r < LANES, 2 * r, 2 * (r - LANES) + 1)
    perm = jnp.where(pick == c, 1.0, 0.0).astype(BF16)
    per_side = side // LANES
    for h in range(PARTS):
        for c in range(tiles):
            map_copy(h, c).wait()

        def separate(t, carry):
            at = pl.multiple_of(h * kpart + t * LANES, LANES)
            for c in range(0, tiles, 2):
                v = jnp.concatenate([
                    stage.at[c + j].reshape(2 * k, LANES)[pl.ds(pl.multiple_of(2 * at, 2 * LANES), 2 * LANES), :]
                    for j in range(2)], axis=1)
                w = dot(perm, v).astype(BF16)
                for j in range(2):
                    s, t = divmod(c + j, per_side)
                    for b in range(2):
                        col = (2 * s + b) * side + t * LANES
                        table[pl.ds(at, LANES), col:col + LANES] = (
                            w[b * LANES:(b + 1) * LANES, j * LANES:(j + 1) * LANES])
            return carry

        lax.fori_loop(0, kpart // LANES, separate, 0)

    def write_ap(s, re, im):
        apbuf[0, :, s * side:(s + 1) * side] = re
        apbuf[1, :, s * side:(s + 1) * side] = im

    wide_product(write_ap)
    pack_corners(lambda at: apbuf[:, :, at:at + LANES].reshape(rows, LANES), cbuf.at[ap_slot])
    send(ap_slot, apbuf)

    def slot_of(n, g):
        return lax.rem(n, 2) * groups + g

    def step(n, g, i, corrected, before):
        wait_in(slot_of(n - 1, g), abuf.at[g])
        assemble(slot_of(n - 1, g), store_lhs)
        restrict_start(i)
        wait_sent(slot_of(n - 1, g), abuf.at[g])
        for s in range(4):
            at = s * side
            w = dot(lhs[:rows], table[:, cols(s)])
            re, im = combine(w)
            abuf[g, 0, :, at:at + side] = re + src_ref[0, g * gs:(g + 1) * gs, at:at + side]
            abuf[g, 1, :, at:at + side] = im + src_ref[1, g * gs:(g + 1) * gs, at:at + side]
        before()
        if corrected:
            for s in range(4):
                at = s * side
                w = dot(ext_lhs[g], ext_rhs[:, cols(s)])
                re, im = combine(w)
                abuf[g, 0, :, at:at + side] += re
                abuf[g, 1, :, at:at + side] += im
        slot = slot_of(n, g)
        pack_corners(lambda at: abuf[g, :, :, at:at + LANES].reshape(rows, LANES), cbuf.at[slot])
        send(slot, abuf.at[g])

    depth = 4
    total = groups * (iters - 1) + 1
    order = [(1, g) for g in range(groups)] + [None]
    order += [(n, g) for n in range(2, iters) for g in range(groups)]

    def small(i):
        if i >= 1:
            restrict_turn((i - 1) % depth)
        if i >= 2:
            finish(i - 2)

    def finish(i):
        if order[i] is None:
            feedback(i % depth)
        else:
            coarse(i % depth, order[i][1])

    for i in range(groups):
        step(1, i, i % depth, False, functools.partial(small, i))

    i = groups
    wait_in(ap_slot, apbuf)
    assemble(ap_slot, store_lhs)
    restrict_start(i % depth)
    for s in range(4):
        at = s * side
        v = (lhs[:rows, at:at + side].astype(F32) + lhs[rows:, at:at + side].astype(F32))
        stack_rhs(eap_rhs, s, v[:nc], v[nc:])
    small(i)
    wide_product(functools.partial(stack_rhs, ext_rhs))

    for g in range(groups):
        i = groups + 1 + g
        step(2, g, i % depth, True, functools.partial(small, i))

    def body(n, carry):
        for g in range(groups):
            i = groups + 1 + (n - 2) * groups + g

            def before():
                restrict_turn(lax.rem(i - 1, depth))
                coarse(lax.rem(i - 2, depth), (g - 2) % groups)

            step(n, g, lax.rem(i, depth), True, before)
        return carry

    lax.fori_loop(3, iters, body, 0)

    restrict_turn((total - 1) % depth)
    for g in range(groups):
        i = total - groups + g
        c_re, c_im = coarse(i % depth, g)
        coef_ref[0, g * gs:(g + 1) * gs] = c_re[:, :nc]
        coef_ref[1, g * gs:(g + 1) * gs] = c_im[:, :nc]
        for s in range(4):
            at = s * side
            w = dot(ext_lhs[g], eap_rhs[:, cols(s)])
            re, im = combine(w)
            traces_ref[0, g * gs:(g + 1) * gs, at:at + side] = re
            traces_ref[1, g * gs:(g + 1) * gs, at:at + side] = im
        slot = ((iters - 1) % 2) * groups + g
        wait_in(slot, abuf.at[g])

        def store_out(at, v):
            traces_ref[:, g * gs:(g + 1) * gs, at:at + LANES] += v.reshape(2, gs, LANES)

        assemble(slot, store_out)
    for g in range(groups):
        wait_sent(((iters - 1) % 2) * groups + g, abuf.at[g])
    wait_sent(ap_slot, apbuf)


def per_device(ny, nx, interface_map, source_trace, restriction, prolongation, coarse_inverse):
    _, _, _, nsrc, _, side = source_trace.shape
    nc = restriction.shape[3]
    k, rows = 4 * side, 2 * nc
    tiles = k // LANES
    groups = nsrc // nc
    slots = 2 * groups + 1
    half = nc // 2
    table = interface_map.reshape(k, 2, tiles, LANES).transpose(0, 2, 1, 3)
    src = source_trace.reshape(2, nsrc, k)
    rest = restriction.reshape(rows, k)
    lift = prolongation.reshape(rows, k)
    dma = pltpu.SemaphoreType.DMA
    vmem = pl.BlockSpec(memory_space=pltpu.VMEM)
    depth = 4
    traces, coef = pl.pallas_call(
        functools.partial(sweep_kernel, ny, nx, ITERS),
        out_shape=(
            jax.ShapeDtypeStruct((2, nsrc, k), F32),
            jax.ShapeDtypeStruct((2, nsrc, nc), F32),
        ),
        in_specs=[pl.BlockSpec(memory_space=pl.ANY)] + [vmem] * 4,
        out_specs=(vmem, vmem),
        scratch_shapes=[
            pltpu.VMEM((tiles, k, 2, LANES), BF16),
            pltpu.VMEM((k, 2 * k), BF16),
            pltpu.VMEM((groups, 2, nc, k), F32),
            pltpu.VMEM((2, nc, k), F32),
            pltpu.VMEM((slots, 2, nc, k), F32),
            pltpu.VMEM((slots, 8, LANES), F32),
            pltpu.VMEM((slots, 4, 8, LANES), F32),
            pltpu.VMEM((2 * rows, k), BF16),
            pltpu.VMEM((groups, rows, LANES), BF16),
            pltpu.VMEM((LANES, 2 * k), BF16),
            pltpu.VMEM((LANES, 2 * k), BF16),
            pltpu.VMEM((2 * rows, k), BF16),
            pltpu.VMEM((depth, half, LANES), F32),
            pltpu.VMEM((depth, nx, half, LANES), F32),
            pltpu.VMEM((depth, half, LANES), F32),
            pltpu.VMEM((depth, ny, half, LANES), F32),
            pltpu.VMEM((2, 2 * LANES, LANES), F32),
            pltpu.VMEM((groups, nc, LANES), F32),
            dma((slots, 4)), dma((slots, 4)), dma((slots, 4)), dma((slots, 4)),
            dma((depth, nx)), dma((depth, nx)), dma((depth, ny)), dma((depth, ny)),
            dma((PARTS, tiles)),
        ],
        compiler_params=pltpu.CompilerParams(
            has_side_effects=True, vmem_limit_bytes=56 * 1024 * 1024
        ),
    )(table, src, rest, lift, coarse_inverse)
    return (
        traces.reshape(source_trace.shape),
        coef,
    )


def solution(mesh):
    return jax.shard_map(
        functools.partial(per_device, mesh.shape["sy"], mesh.shape["sx"]),
        mesh=mesh,
        in_specs=(
            P(("wl", "sy"), "sx", None, None, None),
            P(("wl", "sy"), "sx", None, None, None, None),
            P(("wl", "sy"), "sx", None, None, None, None),
            P(("wl", "sy"), "sx", None, None, None, None),
            P("wl", None, None),
        ),
        out_specs=(P(("wl", "sy"), "sx", None, None, None, None), P("wl", None, None)),
        check_vma=False,
    )
```

```python
import functools

import jax
import jax.numpy as jnp
from jax import lax
from jax.experimental import pallas as pl
from jax.experimental.pallas import tpu as pltpu
from jax.sharding import PartitionSpec as P

ITERS = 6
LANES = 128
F32, BF16 = jnp.float32, jnp.bfloat16
MESH = pl.DeviceIdType.MESH
PRECISE = lax.Precision.HIGHEST
NT = (((1,), (1,)), ((), ()))
PARTS = 4


def dot(a, b):
    return jnp.dot(a, b, preferred_element_type=F32)


def dot_nt(a, b):
    return lax.dot_general(a, b, NT, preferred_element_type=F32)


def split(x):
    hi = x.astype(BF16)
    return hi, (x - hi.astype(F32)).astype(BF16)


def sweep_kernel(
    ny, nx, iters,
    map_hbm, src_in, rest_in, lift_in, inv_ref,
    traces_ref, coef_ref,
    src_ref, stage, table, abuf, apbuf, recv, cbuf, crecv, lhs, ext_lhs, ext_rhs, eap_rhs,
    wts, part, xs, rowsum, ys, inv_full, prev,
    side_send, side_recv, diag_send, diag_recv,
    x_send, x_recv, y_send, y_recv, map_sem,
):
    _, nsrc, k = src_ref.shape
    side = k // 4
    nc = rest_in.shape[1]
    rows = 2 * nc
    gs = nc
    groups = nsrc // gs
    tiles = k // LANES
    half = gs // 2
    ap_slot = 2 * groups
    y, x = lax.axis_index("sy"), lax.axis_index("sx")
    up, dn, lf, rt = y > 0, y < ny - 1, x > 0, x < nx - 1
    odd = lax.rem(y, 2) == 1
    sides = ((up, -1, 0), (dn, 1, 0), (lf, 0, -1), (rt, 0, 1))
    diags = (
        (up & lf, -1, -1),
        (up & rt, -1, 1),
        (dn & lf, 1, -1),
        (dn & rt, 1, 1),
    )

    def lanes(s):
        return pl.ds(s * side, side)

    kpart = k // PARTS

    def map_copy(h, c):
        at = pl.ds(h * kpart, kpart)
        return pltpu.make_async_copy(map_hbm.at[at, c], stage.at[c, at], map_sem.at[h, c])

    for h in range(PARTS):
        for c in range(tiles):
            map_copy(h, c).start()

    def exchange(slot, src):
        flat, diag, flat_in, diag_in = [], [], [], []
        for d, (cond, dy, dx) in enumerate(sides):
            o = d ^ 1
            dev = {"sy": y + dy, "sx": x + dx}
            flat.append((cond, pltpu.make_async_remote_copy(
                src.at[:, :, lanes(d)], recv.at[slot, :, :, lanes(o)],
                side_send.at[slot, d], side_recv.at[slot, o],
                device_id=dev, device_id_type=MESH)))
            flat_in.append((cond, pltpu.make_async_remote_copy(
                src.at[:, :, lanes(d)], recv.at[slot, :, :, lanes(d)],
                side_send.at[slot, d], side_recv.at[slot, d],
                device_id=dev, device_id_type=MESH)))
        for d, (cond, dy, dx) in enumerate(diags):
            o = 3 - d
            dev = {"sy": y + dy, "sx": x + dx}
            diag.append((cond, pltpu.make_async_remote_copy(
                cbuf.at[slot], crecv.at[slot, o], diag_send.at[slot, d], diag_recv.at[slot, o],
                device_id=dev, device_id_type=MESH)))
            diag_in.append((cond, pltpu.make_async_remote_copy(
                cbuf.at[slot], crecv.at[slot, d], diag_send.at[slot, d], diag_recv.at[slot, d],
                device_id=dev, device_id_type=MESH)))
        return flat, diag, flat_in, diag_in

    def each(items, what):
        for cond, c in items:
            pl.when(cond)(getattr(c, what))

    def send(slot, src):
        flat, diag, _, _ = exchange(slot, src)
        each(diag, "start")
        (_, north), (_, south), west, east = flat
        pl.when(dn & odd)(south.start)
        pl.when(up)(north.start)
        pl.when(dn & jnp.logical_not(odd))(south.start)
        each((west, east), "start")

    def wait_in(slot, src):
        _, _, flat_in, diag_in = exchange(slot, src)
        each(diag_in, "wait_recv")
        each(flat_in, "wait_recv")

    def wait_sent(slot, src):
        flat, diag, _, _ = exchange(slot, src)
        each(flat, "wait_send")
        each(diag, "wait_send")

    def pack_corners(read, dst):
        def column(s, last):
            if last:
                return read((s + 1) * side - LANES)[:, LANES - 1:]
            return read(s * side)[:, 0:1]

        lane = lax.broadcasted_iota(jnp.int32, (rows, LANES), 1)
        block = jnp.zeros((rows, LANES), F32)
        for j, (a, b) in enumerate((
            ((0, 0), (2, 0)), ((0, 1), (3, 0)), ((1, 0), (2, 1)), ((1, 1), (3, 1)),
        )):
            block = jnp.where(lane == j, column(*a) + column(*b), block)
        if rows < LANES:
            block = jnp.concatenate([block, jnp.zeros((LANES - rows, LANES), F32)], axis=0)
        dst[...] = block.T[:8]

    def assemble(slot, write):
        row = lax.broadcasted_iota(jnp.int32, (LANES, LANES), 0)
        block = jnp.zeros((LANES, LANES), F32)
        for j in range(4):
            block = jnp.where(row == j, crecv[slot, j][3 - j:4 - j], block)
        cols = block.T[:rows] * 0.5
        lane = lax.broadcasted_iota(jnp.int32, (rows, LANES), 1)
        ends = ((0, 1), (2, 3), (0, 2), (1, 3))
        for s in range(4):
            for t in range(side // LANES):
                at = s * side + t * LANES
                v = recv[slot, :, :, at:at + LANES].reshape(rows, LANES)
                if t == 0:
                    j = ends[s][0]
                    v = v + jnp.where(lane == 0, cols[:, j:j + 1], 0.0)
                if t == side // LANES - 1:
                    j = ends[s][1]
                    v = v + jnp.where(lane == LANES - 1, cols[:, j:j + 1], 0.0)
                write(at, v)

    def joined(ref, n):
        return jnp.concatenate([ref[t, :n] for t in range(tiles)], axis=1)

    def store_lhs(at, v):
        hi, lo = split(v)
        lhs[at // LANES, :rows] = hi
        lhs[at // LANES, rows:] = lo

    def x_copies(i):
        res = []
        for d in range(1, nx):
            dev = {"sy": y, "sx": lax.rem(x + d, nx)}
            res.append((
                pltpu.make_async_remote_copy(
                    part.at[i], xs.at[i, x], x_send.at[i, d], x_recv.at[i, d],
                    device_id=dev, device_id_type=MESH),
                pltpu.make_async_remote_copy(
                    part.at[i], xs.at[i, lax.rem(x + nx - d, nx)], x_send.at[i, d], x_recv.at[i, d],
                    device_id=dev, device_id_type=MESH)))
        return res

    def y_copies(i):
        res = []
        for d in range(1, ny):
            dev = {"sy": lax.rem(y + d, ny), "sx": x}
            res.append((
                pltpu.make_async_remote_copy(
                    rowsum.at[i], ys.at[i, y], y_send.at[i, d], y_recv.at[i, d],
                    device_id=dev, device_id_type=MESH),
                pltpu.make_async_remote_copy(
                    rowsum.at[i], ys.at[i, lax.rem(y + ny - d, ny)], y_send.at[i, d], y_recv.at[i, d],
                    device_id=dev, device_id_type=MESH)))
        return res

    def restrict_start(i):
        t = dot_nt(joined(lhs, 2 * rows), joined(wts, 2 * rows))
        t = t[:rows] + t[rows:]
        t = t + pltpu.roll(t, 2 * nc, 1)
        im = pltpu.roll(t[gs:], nc, 1)
        lane = lax.broadcasted_iota(jnp.int32, (gs, LANES), 1)
        t = t[:gs] + jnp.where((lane < nc) | ((lane >= 2 * nc) & (lane < 3 * nc)), -im, im)
        lane = lax.broadcasted_iota(jnp.int32, (half, LANES), 1)
        t = jnp.where(lane < 2 * nc, t[:half], t[half:])
        part[i] = t
        xs[i, x] = t
        for c, _ in x_copies(i):
            c.start()

    def restrict_turn(i):
        for _, c in x_copies(i):
            c.wait_recv()
        t = xs[i, 0]
        for j in range(1, nx):
            t = t + xs[i, j]
        rowsum[i] = t
        ys[i, y] = t
        for c, _ in y_copies(i):
            c.start()

    def restrict_end(i):
        for _, c in y_copies(i):
            c.wait_recv()
        for c, _ in x_copies(i):
            c.wait_send()
        for c, _ in y_copies(i):
            c.wait_send()
        t = ys[i, 0]
        for j in range(1, ny):
            t = t + ys[i, j]
        lane = lax.broadcasted_iota(jnp.int32, (half, LANES), 1)
        low = lane < 2 * nc
        return jnp.concatenate([jnp.where(low, t, 0.0), jnp.where(low, 0.0, t)], axis=0)

    def coarse(i, g):
        t = jnp.concatenate([restrict_end(i), prev[g]], axis=1)
        c_re = jnp.dot(t, inv_full[0], preferred_element_type=F32, precision=PRECISE)
        c_im = jnp.dot(t, inv_full[1], preferred_element_type=F32, precision=PRECISE)
        lane = lax.broadcasted_iota(jnp.int32, (gs, LANES), 1)
        prev[g] = jnp.where(lane < nc, c_re, jnp.where(lane < 2 * nc, c_im, 0.0))
        c = jnp.concatenate([c_re, c_im], axis=0)
        hi, lo = split(c)
        lane = lax.broadcasted_iota(jnp.int32, (rows, LANES), 1)
        mid = (lane >= nc) & (lane < 2 * nc)
        ext_lhs[g] = jnp.where(mid, lo.astype(F32), hi.astype(F32)).astype(BF16)
        return c_re, c_im

    def feedback(i):
        t = restrict_end(i)
        g_re = jnp.dot(t, inv_full[0, :LANES], preferred_element_type=F32, precision=PRECISE)
        g_im = jnp.dot(t, inv_full[1, :LANES], preferred_element_type=F32, precision=PRECISE)
        inv_full[0, LANES:LANES + nc] = g_re
        inv_full[0, LANES + nc:LANES + 2 * nc] = -g_im
        inv_full[1, LANES:LANES + nc] = g_im
        inv_full[1, LANES + nc:LANES + 2 * nc] = g_re

    def combine(w):
        p, q = w[:, :LANES], w[:, LANES:]
        return p[:nc] - q[nc:], q[:nc] + p[nc:]

    def pair(ref, c):
        return jnp.concatenate([ref[2 * c], ref[2 * c + 1]], axis=1)

    def wide_product(write):
        a = joined(lhs, 2 * rows)
        for c in range(tiles):
            w = dot(a, pair(table, c))
            re, im = combine(w[:rows] + w[rows:])
            write(c, re, im)

    def stack_rhs(dst, c, re, im):
        for b, v in ((0, re), (1, im)):
            hi, lo = split(v)
            dst[2 * c + b] = jnp.concatenate(
                [hi, hi, lo, jnp.zeros((LANES - 3 * nc, LANES), BF16)], axis=0)

    for d, (cond, _, _) in enumerate(sides):
        @pl.when(jnp.logical_not(cond))
        def _(d=d):
            for slot in range(2 * groups + 1):
                recv[slot, :, :, lanes(d)] = jnp.zeros((2, gs, side), F32)
    for d, (cond, _, _) in enumerate(diags):
        @pl.when(jnp.logical_not(cond))
        def _(d=d):
            for slot in range(2 * groups + 1):
                crecv[slot, d] = jnp.zeros((8, LANES), F32)

    def source(g):
        return src_ref.at[:, pl.ds(g * gs, gs)]

    def native(ref, at):
        n = ref.shape[0] * ref.shape[1]
        s, t = divmod(at // LANES, side // LANES)
        return ref.reshape(n * tiles, LANES)[pl.ds(4 * t + s, n, stride=tiles), :]

    for c in range(tiles):
        at = c * LANES
        src_ref[:, :, at:at + LANES] = native(src_in, at).reshape(2, nsrc, LANES)

    for g in range(groups):
        pack_corners(
            lambda at, g=g: src_ref[:, g * gs:(g + 1) * gs, at:at + LANES].reshape(rows, LANES),
            cbuf.at[g])
        send(g, source(g))

    cr, ci = inv_ref[0], inv_ref[1]
    blank = jnp.zeros((nc, LANES - 3 * nc), F32)
    for i, (top, bottom) in enumerate(((cr, -ci), (ci, cr))):
        for j, v in enumerate((top, bottom, top, bottom)):
            inv_full[i, j * nc:(j + 1) * nc] = jnp.concatenate([v, v, v, blank], axis=1)
        inv_full[i, LANES:] = jnp.zeros((LANES, LANES), F32)
    prev[...] = jnp.zeros_like(prev)
    for t in range(tiles):
        hi, lo = split(native(rest_in, t * LANES))
        wts[t, :rows] = hi
        wts[t, rows:] = lo
    for t in range(tiles):
        store_lhs(t * LANES, native(lift_in, t * LANES))

    r = lax.broadcasted_iota(jnp.int32, (2 * LANES, 2 * LANES), 0)
    c = lax.broadcasted_iota(jnp.int32, (2 * LANES, 2 * LANES), 1)
    pick = jnp.where(r < LANES, 2 * r, 2 * (r - LANES) + 1)
    perm = jnp.where(pick == c, 1.0, 0.0).astype(BF16)
    for h in range(PARTS):
        for c in range(tiles):
            map_copy(h, c).wait()

        def separate(t, carry):
            at = pl.multiple_of(h * kpart + t * LANES, LANES)
            for c in range(0, tiles, 2):
                v = jnp.concatenate([
                    stage.at[c + j].reshape(2 * k, LANES)[pl.ds(pl.multiple_of(2 * at, 2 * LANES), 2 * LANES), :]
                    for j in range(2)], axis=1)
                w = dot(perm, v).astype(BF16)
                for j in range(2):
                    for b in range(2):
                        table[2 * (c + j) + b, pl.ds(at, LANES)] = (
                            w[b * LANES:(b + 1) * LANES, j * LANES:(j + 1) * LANES])
            return carry

        lax.fori_loop(0, kpart // LANES, separate, 0)

    def write_ap(c, re, im):
        apbuf[0, :, c * LANES:(c + 1) * LANES] = re
        apbuf[1, :, c * LANES:(c + 1) * LANES] = im

    wide_product(write_ap)
    pack_corners(lambda at: apbuf[:, :, at:at + LANES].reshape(rows, LANES), cbuf.at[ap_slot])
    send(ap_slot, apbuf)

    def slot_of(n, g):
        return lax.rem(n, 2) * groups + g

    def step(n, g, i, corrected, before):
        wait_in(slot_of(n - 1, g), abuf.at[g])
        assemble(slot_of(n - 1, g), store_lhs)
        restrict_start(i)
        wait_sent(slot_of(n - 1, g), abuf.at[g])
        a = joined(lhs, rows)
        for c in range(tiles):
            at = c * LANES
            re, im = combine(dot(a, pair(table, c)))
            abuf[g, 0, :, at:at + LANES] = re + src_ref[0, g * gs:(g + 1) * gs, at:at + LANES]
            abuf[g, 1, :, at:at + LANES] = im + src_ref[1, g * gs:(g + 1) * gs, at:at + LANES]
        before()
        if corrected:
            e = ext_lhs[g]
            for c in range(tiles):
                at = c * LANES
                re, im = combine(dot(e, pair(ext_rhs, c)))
                abuf[g, 0, :, at:at + LANES] += re
                abuf[g, 1, :, at:at + LANES] += im
        slot = slot_of(n, g)
        pack_corners(lambda at: abuf[g, :, :, at:at + LANES].reshape(rows, LANES), cbuf.at[slot])
        send(slot, abuf.at[g])

    depth = 4
    total = groups * (iters - 1) + 1
    order = [(1, g) for g in range(groups)] + [None]
    order += [(n, g) for n in range(2, iters) for g in range(groups)]

    def small(i):
        if i >= 1:
            restrict_turn((i - 1) % depth)
        if i >= 2:
            finish(i - 2)

    def finish(i):
        if order[i] is None:
            feedback(i % depth)
        else:
            coarse(i % depth, order[i][1])

    for i in range(groups):
        step(1, i, i % depth, False, functools.partial(small, i))

    i = groups
    wait_in(ap_slot, apbuf)
    assemble(ap_slot, store_lhs)
    restrict_start(i % depth)
    for c in range(tiles):
        v = lhs[c, :rows].astype(F32) + lhs[c, rows:].astype(F32)
        stack_rhs(eap_rhs, c, v[:nc], v[nc:])
    small(i)
    wide_product(functools.partial(stack_rhs, ext_rhs))

    for g in range(groups):
        i = groups + 1 + g
        step(2, g, i % depth, True, functools.partial(small, i))

    def body(n, carry):
        for g in range(groups):
            i = groups + 1 + (n - 2) * groups + g

            def before():
                restrict_turn(lax.rem(i - 1, depth))
                coarse(lax.rem(i - 2, depth), (g - 2) % groups)

            step(n, g, lax.rem(i, depth), True, before)
        return carry

    lax.fori_loop(3, iters, body, 0)

    restrict_turn((total - 1) % depth)
    for g in range(groups):
        i = total - groups + g
        c_re, c_im = coarse(i % depth, g)
        coef_ref[0, g * gs:(g + 1) * gs] = c_re[:, :nc]
        coef_ref[1, g * gs:(g + 1) * gs] = c_im[:, :nc]
        e = ext_lhs[g]
        for c in range(tiles):
            at = c * LANES
            re, im = combine(dot(e, pair(eap_rhs, c)))
            traces_ref[0, g * gs:(g + 1) * gs, at:at + LANES] = re
            traces_ref[1, g * gs:(g + 1) * gs, at:at + LANES] = im
        slot = ((iters - 1) % 2) * groups + g
        wait_in(slot, abuf.at[g])

        def store_out(at, v):
            traces_ref[:, g * gs:(g + 1) * gs, at:at + LANES] += v.reshape(2, gs, LANES)

        assemble(slot, store_out)
    for g in range(groups):
        wait_sent(((iters - 1) % 2) * groups + g, abuf.at[g])
    wait_sent(ap_slot, apbuf)


def per_device(ny, nx, interface_map, source_trace, restriction, prolongation, coarse_inverse):
    _, _, _, nsrc, _, side = source_trace.shape
    nc = restriction.shape[3]
    k, rows = 4 * side, 2 * nc
    tiles = k // LANES
    groups = nsrc // nc
    slots = 2 * groups + 1
    half = nc // 2
    table = interface_map.reshape(k, 2, tiles, LANES).transpose(0, 2, 1, 3)

    def by_tiles(v):
        v = v.reshape(2, v.shape[3], 4, side // LANES, LANES)
        return v.transpose(0, 1, 3, 2, 4)

    src, rest, lift = by_tiles(source_trace), by_tiles(restriction), by_tiles(prolongation)
    dma = pltpu.SemaphoreType.DMA
    vmem = pl.BlockSpec(memory_space=pltpu.VMEM)
    depth = 4
    traces, coef = pl.pallas_call(
        functools.partial(sweep_kernel, ny, nx, ITERS),
        out_shape=(
            jax.ShapeDtypeStruct((2, nsrc, k), F32),
            jax.ShapeDtypeStruct((2, nsrc, nc), F32),
        ),
        in_specs=[pl.BlockSpec(memory_space=pl.ANY)] + [vmem] * 4,
        out_specs=(vmem, vmem),
        scratch_shapes=[
            pltpu.VMEM((2, nsrc, k), F32),
            pltpu.VMEM((tiles, k, 2, LANES), BF16),
            pltpu.VMEM((2 * tiles, k, LANES), BF16),
            pltpu.VMEM((groups, 2, nc, k), F32),
            pltpu.VMEM((2, nc, k), F32),
            pltpu.VMEM((slots, 2, nc, k), F32),
            pltpu.VMEM((slots, 8, LANES), F32),
            pltpu.VMEM((slots, 4, 8, LANES), F32),
            pltpu.VMEM((tiles, 2 * rows, LANES), BF16),
            pltpu.VMEM((groups, rows, LANES), BF16),
            pltpu.VMEM((2 * tiles, LANES, LANES), BF16),
            pltpu.VMEM((2 * tiles, LANES, LANES), BF16),
            pltpu.VMEM((tiles, 2 * rows, LANES), BF16),
            pltpu.VMEM((depth, half, LANES), F32),
            pltpu.VMEM((depth, nx, half, LANES), F32),
            pltpu.VMEM((depth, half, LANES), F32),
            pltpu.VMEM((depth, ny, half, LANES), F32),
            pltpu.VMEM((2, 2 * LANES, LANES), F32),
            pltpu.VMEM((groups, nc, LANES), F32),
            dma((slots, 4)), dma((slots, 4)), dma((slots, 4)), dma((slots, 4)),
            dma((depth, nx)), dma((depth, nx)), dma((depth, ny)), dma((depth, ny)),
            dma((PARTS, tiles)),
        ],
        compiler_params=pltpu.CompilerParams(
            has_side_effects=True, vmem_limit_bytes=56 * 1024 * 1024
        ),
    )(table, src, rest, lift, coarse_inverse)
    return (
        traces.reshape(source_trace.shape),
        coef,
    )


def solution(mesh):
    return jax.shard_map(
        functools.partial(per_device, mesh.shape["sy"], mesh.shape["sx"]),
        mesh=mesh,
        in_specs=(
            P(("wl", "sy"), "sx", None, None, None),
            P(("wl", "sy"), "sx", None, None, None, None),
            P(("wl", "sy"), "sx", None, None, None, None),
            P(("wl", "sy"), "sx", None, None, None, None),
            P("wl", None, None),
        ),
        out_specs=(P(("wl", "sy"), "sx", None, None, None, None), P("wl", None, None)),
        check_vma=False,
    )
```
